32 devices in a mesh: grp: 4 (over y, x), dev: 8 (over z, core).
Axes of the slice: x: 2, y: 2, z: 4, core: 2. Of those that a mesh axis runs over, the one named last changes fastest.
Arguments:
- pool_rows: bfloat16 [32768, 1024], P(('grp', 'dev')), may hold values from -6 to 6
- sample_index: int32 [32768], P(('grp', 'dev')), may hold values from 0 to 32767, as said below
- cluster_id: int32 [32768], P(('grp', 'dev')), may hold values from 0 to 63, as said below
- child_id: int32 [32768], P(('grp', 'dev')), may hold values from 0 to 7
- old_centroids: float32 [64, 8, 1024], P('dev'), may hold values from -6 to 6
Outputs:
- centroids: float32 [64, 8, 1024], P('dev')
- child_counts: int32 [64, 8], P('dev')
The draws below stay inside these ranges and needn't reach their ends.
Inputs may be any that keep to these rules, and one draw needn't show every extreme that they name: Sample i takes a pool row of its own aligned block of 1024 rows: sample_index[i] // 1024 == i // 1024. `cluster_id`: in each aligned block of 1024 samples (the rows of one device) the 2 clusters o * 2 to o * 2 + 1 of any owner o are named at most 64 times together, and one cluster, the same in every block, is named exactly 64 times in every block.
All inputs are finite; a program needn't handle non-finite values.
Results may differ from the reference program's by a relative error of at most 0.0003.
Values may be sent and summed in bfloat16 or wider, within the bound.
A program may use at most 64 MiB of HBM per device.

```python
import jax
import jax.numpy as jnp
from jax import lax

D = 1024
KC = 8
CL_DEV = 2
R_DEV = 1024
CLUSTERS = 64
ROWS = 32768
MOST = 64


def shuffle_row(subkey, values):
    return jax.random.permutation(subkey, values)


def draw_cluster_id(key, part):
    blocks = ROWS // R_DEV
    holder_tally_overall = CLUSTERS // CL_DEV
    slots = holder_tally_overall * MOST
    full_key = jax.random.fold_in(key, 11)
    favour_noise_seed = jax.random.fold_in(key, 12)
    noise_key = jax.random.fold_in(key, 13)
    order_key = jax.random.fold_in(key, 14)
    pick_key = jax.random.fold_in(key, 15)
    favoured = jax.random.randint(full_key, (), 0, CLUSTERS)
    favourite_holder_position = favoured // CL_DEV
    holder_advantage = jax.random.randint(favour_noise_seed, (holder_tally_overall,), 0, 4)
    uniform_perturbation = jax.random.randint(noise_key, (blocks, slots), 0, 16384)
    holder_table = (jnp.arange(slots) // MOST).astype(jnp.int32)
    holder_merit = uniform_perturbation + holder_advantage[holder_table][None, :] * 4096 + jnp.where(holder_table == favourite_holder_position, 65536, 0)[None, :]
    holder_merit = (holder_merit * slots + jnp.arange(slots)[None, :]).astype(jnp.int32)
    unused, chosen = lax.top_k(holder_merit, R_DEV)
    keys = jax.random.split(order_key, blocks)
    mixed = jax.vmap(shuffle_row)(keys, chosen.astype(jnp.int32))
    owner = (mixed // MOST).astype(jnp.int32)
    pick = jax.random.randint(pick_key, (blocks, R_DEV), 0, CL_DEV)
    cluster = owner * CL_DEV + pick
    cluster = jnp.where(owner == favourite_holder_position, favoured, cluster)
    return cluster.reshape(-1).astype(jnp.int32)


def draw_sample_index(key, part):
    offset_key = jax.random.fold_in(key, 21)
    within = jax.random.randint(offset_key, (ROWS,), 0, R_DEV)
    base = jnp.arange(ROWS) // R_DEV * R_DEV
    return (base + within).astype(jnp.int32)


def place_ends(entries, rng, low, top_value):
    longest = entries.shape.index(max(entries.shape))
    spots = []
    for shift in (0, 1):
        where = [jax.random.randint(jax.random.fold_in(rng, axis), (), 0, length) for axis, length in enumerate(entries.shape)]
        where[longest] = (where[longest] + shift) % entries.shape[longest]
        spots.append(tuple(where))
    return entries.at[spots[0]].set(low).at[spots[1]].set(top_value)


def shard_levels(key, shape, shards, least, largest):
    def one(dim, blocks):
        draws = jax.random.uniform(jax.random.fold_in(jax.random.fold_in(key, 6), dim), (blocks,), jnp.float32, least / len(shards), largest / len(shards))
        return jnp.repeat(jnp.exp(draws), shape[dim] // blocks).reshape((-1,) + (1,) * (len(shape) - dim - 1))

    gain = one(*shards[0])
    for cut in shards[1:]:
        gain = gain * one(*cut)
    return gain


def scatter_about(stream_key, dims, spread, most, pieces=(), dtype=jnp.bfloat16):
    loudness = shard_levels(stream_key, dims, pieces, -0.22, 0.18) if pieces else 1.0
    drawn = jax.random.normal(stream_key, dims, jnp.float32) * spread * loudness
    return jnp.minimum(jnp.maximum(drawn, -most), most).astype(dtype)


def setup_inputs(seed: int = 0) -> dict:
    arg_keys = jax.random.split(jax.random.key(seed), 6)
    pool_rows = scatter_about(arg_keys[0], (ROWS, D), 1.0, 6.0, ((0, 32),))
    sample_index = draw_sample_index(jax.random.fold_in(arg_keys[5], 71), 0)
    cluster_id = draw_cluster_id(jax.random.fold_in(arg_keys[5], 71), 0)
    child_id = place_ends(jax.random.randint(arg_keys[3], (ROWS,), 0, KC), jax.random.fold_in(arg_keys[3], 1), 0, KC - 1).astype(jnp.int32)
    old_centroids = scatter_about(arg_keys[4], (CLUSTERS, KC, D), 1.0, 6.0, ((0, 8),), jnp.float32)
    return dict(pool_rows=pool_rows, sample_index=sample_index, cluster_id=cluster_id, child_id=child_id, old_centroids=old_centroids)


def reference(pool_rows, sample_index, cluster_id, child_id, old_centroids):
    blocks = ROWS // R_DEV
    segments = CLUSTERS * KC

    def add_block(carry, items):
        sums, counts = carry
        index_block, cluster_block, child_block = items
        rows = pool_rows[index_block].astype(jnp.float32)
        segment = (cluster_block * KC + child_block).astype(jnp.int32)
        sums = sums + jax.ops.segment_sum(rows, segment, num_segments=segments)
        ones = jnp.ones(segment.shape, jnp.int32)
        counts = counts + jax.ops.segment_sum(ones, segment, num_segments=segments)
        return (sums, counts), None

    initial = (jnp.zeros((segments, D), jnp.float32), jnp.zeros((segments,), jnp.int32))
    items = (sample_index.reshape(blocks, R_DEV), cluster_id.reshape(blocks, R_DEV), child_id.reshape(blocks, R_DEV))
    (sums, counts), unused = lax.scan(add_block, initial, items)
    child_counts = counts.reshape(CLUSTERS, KC)
    divisor = child_counts.astype(jnp.float32)[:, :, None] + 1.0
    centroids = (sums.reshape(CLUSTERS, KC, D) + old_centroids) / divisor
    return (centroids, child_counts)
```

```python
import functools

import jax
import jax.numpy as jnp
from jax import lax
from jax.experimental import pallas as pl
from jax.experimental.pallas import tpu as pltpu
from jax.sharding import PartitionSpec as P

MESH = pl.DeviceIdType.MESH
LANES = 128
PAIR = 256
BLOCK_ROWS = 256
ROUTES = (("h", "xy", "l"), ("x", "lh", "y"), ("y", "lh", "x"), ("l", "xy", "h"), ("x", "y", "lh"), ("l", "xy", "h"), ("y", "x", "lh"), ("xy", "lh"))
TAKES = ((1, 0), (2, 0), (3, 0), (4, 0), (6, 0), (0, 0), (5, 0), (7, 0), (3, 1), (4, 1), (6, 1), (1, 1), (0, 1), (2, 1), (5, 1), (1, 2), (7, 1), (3, 2), (0, 2), (2, 2), (4, 2), (6, 2), (5, 2))


def log2(n):
    assert n & (n - 1) == 0
    return n.bit_length() - 1


def run(count, body):
    if count == 1:
        body(0)
    else:
        lax.fori_loop(0, count, lambda i, c: (body(i), c)[1], 0)


class Plan:
    def __init__(self, groups, devs, held, kinds, rows, width):
        self.groups, self.devs, self.held, self.kinds = groups, devs, held, kinds
        self.rows, self.width = rows, width
        self.clusters = devs * held
        self.own = held // groups
        self.dev_bits, self.grp_bits = log2(devs), log2(groups)
        self.free_bits = log2(self.own)
        self.bits = log2(self.clusters)
        self.steps = self.dev_bits + self.grp_bits
        self.chunks = width // LANES
        letters = {"x": ("grp", 0), "y": ("grp", 1), "l": ("dev", 1), "h": ("dev", 2)}
        core = (("dev", 0),)
        rest = [(("dev", b),) for b in range(3, self.dev_bits)]
        rest += [(("grp", b),) for b in range(2, self.grp_bits)]
        self.order, self.ends = [], []
        for k in range(self.chunks):
            near = [tuple(letters[c] for c in word) for word in ROUTES[k % len(ROUTES)]]
            self.order.append([core] + near + rest)
        self.takes = [(k, 0) for k in range(self.chunks)]
        for start in range(0, self.chunks, len(ROUTES)):
            self.takes += [(start + k, s + 1) for k, s in TAKES if start + k < self.chunks]
        for s in range(len(rest)):
            self.takes += [(k, len(self.order[k]) - len(rest) + s) for k in range(self.chunks)]
        self.base = [item for group in self.order[0] for item in group]
        self.count_order = [core, (("dev", 1), ("dev", 2))]
        self.count_order += [(("dev", b),) for b in range(3, self.dev_bits)]
        self.pieces = max(sum((1 << len(g)) - 1 for g in o) for o in self.order)
        self.count_pieces = sum((1 << len(g)) - 1 for g in self.count_order)

    def cluster_bit(self, item):
        axis, b = item
        return b + (log2(self.held) if axis == "dev" else self.free_bits)

    def moves(self, order):
        order = [item for group in order for item in group]
        where = {item: self.bits - 1 - s for s, item in enumerate(self.base)}
        there = {item: self.bits - 1 - s for s, item in enumerate(order)}
        return [(where[i], there[i]) for i in order] + [(b, b) for b in range(self.free_bits)]


def permute(value, moves):
    total = 0
    for a, b in moves:
        total = total + ((value // (1 << a)) % 2) * (1 << b)
    return total


def kernel(plan, idx_hbm, clu_hbm, chi_hbm, pool_hbm, old_hbm, out_ref, cnt_ref,
           idx_ref, clu_ref, chi_ref, id_sem, pool, old, ihot, a_buf, buf, recv, cbuf, crecv, cex, ag,
           load_sem, send_sem, recv_sem, csend_sem, crecv_sem, ag_send, ag_recv):
    p = plan
    grp, dev = lax.axis_index("grp"), lax.axis_index("dev")

    pairs = ((idx_hbm, idx_ref), (clu_hbm, clu_ref), (chi_hbm, chi_ref))
    ids = [pltpu.make_async_copy(a, b, id_sem.at[i]) for i, (a, b) in enumerate(pairs)]
    for c in ids:
        c.start()
    load_pool = pltpu.make_async_copy(pool_hbm, pool, load_sem.at[0])
    load_pool.start()
    load_old = pltpu.make_async_copy(old_hbm, old, load_sem.at[1])
    load_old.start()

    def flip(index, b):
        return index + (1 << b) - 2 * (1 << b) * ((index // (1 << b)) % 2)

    def partner(group, mask):
        g, d = grp, dev
        for at, (axis, b) in enumerate(reversed(group)):
            if (mask >> at) & 1:
                g, d = (g, flip(d, b)) if axis == "dev" else (flip(g, b), d)
        return (g, d)

    def mate(o):
        other = grp
        for b in range(p.grp_bits):
            if (o >> b) & 1:
                other = flip(other, b)
        return (other, dev)

    named = {}
    for order in p.order + [p.count_order, [tuple(("grp", b) for b in range(p.grp_bits))]]:
        for group in order:
            for mask in range(1, 1 << len(group)):
                picked = [i for at, i in enumerate(reversed(group)) if (mask >> at) & 1]
                named[tuple(sorted(picked))] = (group, mask)
    greeted = [partner(*named[name]) for name in sorted(named)]
    barrier = pltpu.get_barrier_semaphore()
    for other in greeted:
        pl.semaphore_signal(barrier, inc=1, device_id=other, device_id_type=MESH)

    for c in ids:
        c.wait()
    local = idx_ref[...] - (grp * p.devs + dev) * p.rows
    cluster = clu_ref[...]
    child = chi_ref[...]
    relative = jnp.bitwise_xor(cluster, dev * p.held + grp * p.own)

    def label(pairs):
        total = None
        for a, b in pairs:
            term = (lax.shift_right_logical(relative, a) & 1) << b
            total = term if total is None else total + term
        return total

    base_pairs = [(p.cluster_bit(i), p.bits - 1 - s) for s, i in enumerate(p.base)]
    base_pairs += [(b, b) for b in range(p.free_bits)]
    segment = label(base_pairs) * p.kinds + child

    def onehot(rows, start, labels):
        at = lax.broadcasted_iota(jnp.int32, (rows, p.rows), 0) + start
        return jnp.where(at == labels, 1.0, 0.0).astype(jnp.bfloat16)

    def dot_t(a, b):
        return lax.dot_general(a, b, (((1,), (1,)), ((), ())), preferred_element_type=jnp.float32)

    log_held = log2(p.held)
    count_label = label(
        [(log_held + b, p.dev_bits - 1 - s + log_held) for s, (_, b) in
         enumerate([i for g in p.count_order for i in g])]
    ) + cluster % p.held
    hits = dot_t(onehot(p.clusters, 0, count_label), onehot(LANES, 0, child))
    cbuf[...] = hits.reshape(p.devs, p.held, LANES)

    def exchange(src, dst, s_sem, r_sem, device):
        return pltpu.make_async_remote_copy(
            src_ref=src, dst_ref=dst, send_sem=s_sem, recv_sem=r_sem,
            device_id=device, device_id_type=MESH)

    def parts(order, total, s):
        before = sum(len(g) for g in order[:s])
        first = sum((1 << len(g)) - 1 for g in order[:s]) - 1
        n = (total >> before) >> len(order[s])
        return [(m, m * n, n, first + m) for m in range(1, 1 << len(order[s]))]

    def pieces(k, s):
        got = []
        for m, at, n, sem in parts(p.order[k], p.clusters, s):
            span = pl.ds(at, n)
            got.append(exchange(buf.at[k, span], recv.at[k, span], send_sem.at[k, sem],
                                recv_sem.at[k, sem], partner(p.order[k][s], m)))
        return got

    def count_pieces(s):
        if s == len(p.count_order):
            return [exchange(cbuf.at[0], cex.at[o - 1], csend_sem.at[p.count_pieces + o - 1],
                             crecv_sem.at[p.count_pieces + o - 1], mate(o))
                    for o in range(1, p.groups)]
        got = []
        for m, at, n, sem in parts(p.count_order, p.devs, s):
            span = pl.ds(at, n)
            got.append(exchange(cbuf.at[span], crecv.at[span], csend_sem.at[sem],
                                crecv_sem.at[sem], partner(p.count_order[s], m)))
        return got

    def start(copies):
        for copy in copies:
            copy.start()

    def take_count(s):
        for copy in count_pieces(s):
            copy.wait_recv()
        todo = parts(p.count_order, p.devs, s)
        n = todo[0][2]
        total = cbuf[0:n]
        for _, at, n, _ in todo:
            total = total + crecv[at:at + n]
        cbuf[0:n] = total
        start(count_pieces(s + 1))

    mine = pl.ds(grp * p.own, p.own)

    def gather(k):
        return [exchange(buf.at[k, 0:p.own], ag.at[k, mine], ag_send.at[k, o - 1],
                         ag_recv.at[k, o - 1], mate(o)) for o in range(1, p.groups)]

    def take(k, s):
        for copy in pieces(k, s):
            copy.wait_recv()
        todo = parts(p.order[k], p.clusters, s)
        n = todo[0][2]
        total = buf[k, 0:n]
        for _, at, n, _ in todo:
            total = total + recv[k, at:at + n]
        buf[k, 0:n] = total
        if s + 1 < len(p.order[k]):
            start(pieces(k, s + 1))
        else:
            start(gather(k))
            ag[k, mine] = total

    ihot[...] = onehot(p.rows, 0, local)
    half_rows = p.clusters * p.kinds // 2
    block = min(BLOCK_ROWS, half_rows)
    blocks = half_rows // block
    block_clusters = block // p.kinds

    for half in (1, 0):

        def rows_of(i):
            return pl.ds(i * block, block)

        def make_a(i):
            hot = onehot(block, half * half_rows + i * block, segment)
            a_buf[rows_of(i), :] = dot_t(hot, ihot[...]).astype(jnp.bfloat16)

        run(blocks, make_a)
        if half == 1:
            load_pool.wait()
        for c in range(p.width // PAIR):

            def multiply(i):
                got = jnp.dot(a_buf[rows_of(i), :], pool[:, c * PAIR:(c + 1) * PAIR],
                              preferred_element_type=jnp.float32)
                got = got.reshape(block_clusters, p.kinds, PAIR)
                for q in range(PAIR // LANES):
                    k = c * (PAIR // LANES) + q
                    moves = p.moves(p.order[k])
                    start = permute((half * half_rows + i * block) // p.kinds, moves)
                    for j in range(block_clusters):
                        buf[k, start + permute(j, moves)] = got[j, :, q * LANES:(q + 1) * LANES]

            run(blocks, multiply)
            if half == 1:
                if c == 0:
                    pl.semaphore_wait(barrier, len(greeted))
                for q in range(PAIR // LANES):
                    start(pieces(c * (PAIR // LANES) + q, 0))

    start(count_pieces(0))
    due = {p.chunks - 1: 0}
    for s in range(1, len(p.count_order)):
        due[len(p.takes) // 2 + s - 1] = s
    for at, (k, s) in enumerate(p.takes):
        take(k, s)
        if at in due:
            take_count(due[at])

    last = len(p.count_order)
    for copy in count_pieces(last):
        copy.wait_recv()
    total = cbuf[0]
    for o in range(1, p.groups):
        total = total + cex[o - 1]
    cnt_ref[...] = total[:, 0:p.kinds].astype(jnp.int32)
    pick = (lax.broadcasted_iota(jnp.int32, (p.held, p.kinds, LANES), 1)
            == lax.broadcasted_iota(jnp.int32, (p.held, p.kinds, LANES), 2))
    spread = jnp.where(pick, total[:, None, :], 0.0)
    divisor = jnp.sum(spread, axis=2, keepdims=True) + 1.0
    load_old.wait()

    ends = [k for k, s in p.takes if s == len(p.order[k]) - 1]
    for k in ends:
        for o in range(1, p.groups):
            theirs = pl.ds(mate(o)[0] * p.own, p.own)
            exchange(buf.at[k, 0:p.own], ag.at[k, theirs], ag_send.at[k, o - 1],
                     ag_recv.at[k, o - 1], mate(o)).wait_recv()
        lanes = slice(k * LANES, (k + 1) * LANES)
        out_ref[:, :, lanes] = (ag[k] + old[:, :, lanes]) / divisor

    for k in range(p.chunks):
        for s in range(len(p.order[k])):
            for copy in pieces(k, s):
                copy.wait_send()
        for copy in gather(k):
            copy.wait_send()
    for s in range(last + 1):
        for copy in count_pieces(s):
            copy.wait_send()


def finish(centroids, counts):
    def body(a_ref, b_ref, c_ref, d_ref):
        c_ref[...] = a_ref[...]
        d_ref[...] = b_ref[...]

    whole = pl.BlockSpec(memory_space=pltpu.VMEM)
    shapes = [jax.ShapeDtypeStruct(a.shape, a.dtype) for a in (centroids, counts)]
    return pl.pallas_call(body, out_shape=tuple(shapes), in_specs=[whole, whole],
                          out_specs=(whole, whole), compiler_params=pltpu.CompilerParams(vmem_limit_bytes=4 * 2**20))(centroids, counts)


def per_device(groups, devs, pool_rows, sample_index, cluster_id, child_id, old_centroids):
    rows, width = pool_rows.shape
    held, kinds, _ = old_centroids.shape
    plan = Plan(groups, devs, held, kinds, rows, width)
    f32, bf16 = jnp.float32, jnp.bfloat16
    whole = pl.BlockSpec(memory_space=pltpu.VMEM)
    stay = pl.BlockSpec(memory_space=pltpu.HBM)
    half_rows = plan.clusters * kinds // 2
    return finish(*pl.pallas_call(
        functools.partial(kernel, plan),
        out_shape=(
            jax.ShapeDtypeStruct((held, kinds, width), f32),
            jax.ShapeDtypeStruct((held, kinds), jnp.int32),
        ),
        in_specs=[stay, stay, stay, stay, stay],
        out_specs=(whole, whole),
        scratch_shapes=[
            pltpu.VMEM((1, rows), jnp.int32),
            pltpu.VMEM((1, rows), jnp.int32),
            pltpu.VMEM((1, rows), jnp.int32),
            pltpu.SemaphoreType.DMA((3,)),
            pltpu.VMEM((rows, width), bf16),
            pltpu.VMEM((held, kinds, width), f32),
            pltpu.VMEM((rows, rows), bf16),
            pltpu.VMEM((half_rows, rows), bf16),
            pltpu.VMEM((plan.chunks, plan.clusters, kinds, LANES), f32),
            pltpu.VMEM((plan.chunks, plan.clusters, kinds, LANES), f32),
            pltpu.VMEM((devs, held, LANES), f32),
            pltpu.VMEM((devs, held, LANES), f32),
            pltpu.VMEM((groups - 1, held, LANES), f32),
            pltpu.VMEM((plan.chunks, held, kinds, LANES), f32),
            pltpu.SemaphoreType.DMA((2,)),
            pltpu.SemaphoreType.DMA((plan.chunks, plan.pieces)),
            pltpu.SemaphoreType.DMA((plan.chunks, plan.pieces)),
            pltpu.SemaphoreType.DMA((plan.count_pieces + groups - 1,)),
            pltpu.SemaphoreType.DMA((plan.count_pieces + groups - 1,)),
            pltpu.SemaphoreType.DMA((plan.chunks, groups - 1)),
            pltpu.SemaphoreType.DMA((plan.chunks, groups - 1)),
        ],
        compiler_params=pltpu.CompilerParams(
            collective_id=0, has_side_effects=True, vmem_limit_bytes=50 * 2**20
        ),
    )(
        *[pltpu.with_memory_space_constraint(a, pltpu.HBM) for a in (sample_index.reshape(1, rows), cluster_id.reshape(1, rows), child_id.reshape(1, rows), pool_rows, old_centroids)],
    ))


def solution(mesh):
    placed = (
        P(("grp", "dev"), None),
        P(("grp", "dev")),
        P(("grp", "dev")),
        P(("grp", "dev")),
        P("dev", None, None),
    )
    return jax.shard_map(
        functools.partial(per_device, mesh.shape["grp"], mesh.shape["dev"]),
        mesh=mesh,
        in_specs=placed,
        out_specs=(P("dev", None, None), P("dev", None)),
        check_vma=False,
    )
```
